32 devices in a mesh: data: 1 (over z), model: 32 (over y, x, core).
Axes of the slice: x: 4, y: 4, z: 1, core: 2. Of those that a mesh axis runs over, the one named last changes fastest.
The devices are a block of a 4x4x8 slice.
Arguments:
- act_x: bfloat16 [4096, 2048], P('data')
- seg_ids: int32 [4096], P('data')
- gain_one: bfloat16 [2048], replicated
- gain_two: bfloat16 [2048], replicated
- w_qkv: bfloat16 [2048, 6144], P(None, 'model')
- w_out: bfloat16 [32, 64, 2048], P('model')
- w_up: bfloat16 [2048, 8192], P(None, 'model')
- w_down: bfloat16 [8192, 2048], P('model')
- grad_y: bfloat16 [4096, 2048], P('data')
Outputs:
- output 1: bfloat16 [4096, 2048], P('data')
- output 2: bfloat16 [4096, 2048], P('data')
- output 3: bfloat16 [2048, 6144], P('data', 'model')
- output 4: bfloat16 [32, 64, 2048], P(('data', 'model'))
- output 5: bfloat16 [2048, 8192], P('data', 'model')
- output 6: bfloat16 [8192, 2048], P(('data', 'model'))
- output 7: bfloat16 [2048], P('data')
- output 8: bfloat16 [2048], P('data')
All inputs are finite; a program needn't handle non-finite values.
Results may differ from the reference program's by a relative error of at most 0.02.
Values are sent between devices in bfloat16 or wider.
A program may use at most 768 MiB of HBM per device.

```python
import jax
import jax.numpy as jnp
from jax import lax

HIDDEN = 2048
NUM_HEADS = 32
HEAD_DIM = 64
FFN_DIM = 8192
SEQ_LEN = 4096
NUM_BOUNDS = 3


def matmul_f32(left, right):
    return jnp.dot(left.astype(jnp.float32), right.astype(jnp.float32))


def layer_norm(values, gain_vec):
    values_f32 = values.astype(jnp.float32)
    centered = values_f32 - jnp.mean(values_f32, axis=-1, keepdims=True)
    variance = jnp.mean(centered * centered, axis=-1, keepdims=True)
    return centered * lax.rsqrt(variance + 1e-5) * gain_vec.astype(jnp.float32)


def setup_inputs(seed: int = 0, part: int = 0) -> dict:
    part_key = jax.random.fold_in(jax.random.key(seed), part)
    key_x, key_dy, key_seg = jax.random.split(part_key, 3)
    weight_keys = jax.random.split(jax.random.key(seed + 1), 6)
    act_x = jax.random.normal(key_x, (SEQ_LEN, HIDDEN), jnp.float32)
    grad_y = jax.random.normal(key_dy, (SEQ_LEN, HIDDEN), jnp.float32)
    bounds = jax.random.randint(key_seg, (NUM_BOUNDS,), 1, SEQ_LEN, dtype=jnp.int32)
    positions = jnp.arange(SEQ_LEN, dtype=jnp.int32)
    seg_ids = jnp.sum((positions[:, None] >= bounds[None, :]).astype(jnp.int32), axis=1).astype(jnp.int32)
    gain_one = 1.0 + 0.3 * jax.random.normal(weight_keys[0], (HIDDEN,), jnp.float32)
    gain_two = 1.0 + 0.3 * jax.random.normal(weight_keys[1], (HIDDEN,), jnp.float32)
    part_scale = jnp.array([1.5, 1.5, 1.0], jnp.float32)
    col_scale = jnp.tile(jnp.repeat(part_scale, HEAD_DIM), NUM_HEADS)
    w_qkv = jax.random.normal(weight_keys[2], (HIDDEN, 3 * NUM_HEADS * HEAD_DIM), jnp.float32) * (HIDDEN ** -0.5) * col_scale
    w_out = jax.random.normal(weight_keys[3], (NUM_HEADS, HEAD_DIM, HIDDEN), jnp.float32) * ((NUM_HEADS * HEAD_DIM) ** -0.5)
    w_up = jax.random.normal(weight_keys[4], (HIDDEN, FFN_DIM), jnp.float32) * (HIDDEN ** -0.5)
    w_down = jax.random.normal(weight_keys[5], (FFN_DIM, HIDDEN), jnp.float32) * (FFN_DIM ** -0.5)
    return {
        "act_x": act_x.astype(jnp.bfloat16),
        "seg_ids": seg_ids,
        "gain_one": gain_one.astype(jnp.bfloat16),
        "gain_two": gain_two.astype(jnp.bfloat16),
        "w_qkv": w_qkv.astype(jnp.bfloat16),
        "w_out": w_out.astype(jnp.bfloat16),
        "w_up": w_up.astype(jnp.bfloat16),
        "w_down": w_down.astype(jnp.bfloat16),
        "grad_y": grad_y.astype(jnp.bfloat16),
    }


def reference(act_x, seg_ids, gain_one, gain_two, w_qkv, w_out, w_up, w_down, grad_y):
    positions = jnp.arange(SEQ_LEN, dtype=jnp.int32)
    allowed = (positions[:, None] >= positions[None, :]) & (seg_ids[:, None] == seg_ids[None, :])

    def one_head(head_rows):
        q_head, k_head, v_head = head_rows
        scores = matmul_f32(q_head, k_head.T) * (HEAD_DIM ** -0.5)
        scores = jnp.where(allowed, scores, -1e30)
        prob_f32 = jax.nn.softmax(scores, axis=-1)
        return matmul_f32(prob_f32.astype(jnp.bfloat16), v_head).astype(jnp.bfloat16)

    head_fn = jax.checkpoint(one_head)

    def layer_map(x_in, g_one, g_two, wqkv_in, wout_in, wup_in, wdown_in):
        normed_one = layer_norm(x_in, g_one).astype(jnp.bfloat16)
        qkv_rows = matmul_f32(normed_one, wqkv_in).astype(jnp.bfloat16)
        qkv_heads = jnp.transpose(qkv_rows.reshape(SEQ_LEN, NUM_HEADS, 3, HEAD_DIM), (2, 1, 0, 3))
        attn_heads = lax.map(head_fn, (qkv_heads[0], qkv_heads[1], qkv_heads[2]))
        attn_rows = jnp.transpose(attn_heads, (1, 0, 2)).reshape(SEQ_LEN, NUM_HEADS * HEAD_DIM)
        attn_proj = matmul_f32(attn_rows, wout_in.reshape(NUM_HEADS * HEAD_DIM, HIDDEN))
        resid_rows = (x_in.astype(jnp.float32) + attn_proj).astype(jnp.bfloat16)
        normed_two = layer_norm(resid_rows, g_two).astype(jnp.bfloat16)
        hidden = jax.nn.gelu(matmul_f32(normed_two, wup_in), approximate=True).astype(jnp.bfloat16)
        return (resid_rows.astype(jnp.float32) + matmul_f32(hidden, wdown_in)).astype(jnp.bfloat16)

    layer_out, pullback = jax.vjp(layer_map, act_x, gain_one, gain_two, w_qkv, w_out, w_up, w_down)
    grads = pullback(grad_y)
    return (layer_out, grads[0], grads[3], grads[4], grads[5], grads[6], grads[1], grads[2])
```

```python
import functools
import math
import jax
import jax.numpy as jnp
from jax import lax
from jax.experimental import pallas as pl
from jax.experimental.pallas import tpu as pltpu
from jax.sharding import PartitionSpec as P

LN_EPS = 1e-5
VMEM_LIMIT = 60 * 1024 * 1024
BQ = 256
BK = 512
NEG = -1e30


def ln_qkv_kernel(x_ref, g_ref, w_ref, a_ref, qkv_ref):
    x = x_ref[...].astype(jnp.float32)
    centered = x - jnp.mean(x, axis=-1, keepdims=True)
    inv_std = lax.rsqrt(jnp.mean(centered * centered, axis=-1, keepdims=True) + LN_EPS)
    a = (centered * inv_std * g_ref[...].astype(jnp.float32)).astype(jnp.bfloat16)
    a_ref[...] = a
    qkv_ref[...] = jnp.dot(a, w_ref[...], preferred_element_type=jnp.float32).astype(jnp.bfloat16)


def ln_qkv(x, gain, w):
    tokens, width = x.shape
    cols = w.shape[1]
    rows = 512
    return pl.pallas_call(
        ln_qkv_kernel,
        grid=(tokens // rows,),
        in_specs=[pl.BlockSpec((rows, width), lambda i: (i, 0)),
                  pl.BlockSpec((1, width), lambda i: (0, 0)),
                  pl.BlockSpec((width, cols), lambda i: (0, 0))],
        out_specs=[pl.BlockSpec((rows, width), lambda i: (i, 0)),
                   pl.BlockSpec((rows, cols), lambda i: (i, 0))],
        out_shape=[jax.ShapeDtypeStruct((tokens, width), jnp.bfloat16),
                   jax.ShapeDtypeStruct((tokens, cols), jnp.bfloat16)],
        compiler_params=pltpu.CompilerParams(vmem_limit_bytes=VMEM_LIMIT),
        cost_estimate=pl.CostEstimate(flops=2 * tokens * width * cols, bytes_accessed=4 * tokens * width,
                                      transcendentals=0),
        name="ln_qkv",
    )(x, gain[None, :], w)


def _mask(i, j, start):
    shape = (BQ, BK)
    row = lax.broadcasted_iota(jnp.int32, shape, 0) + i * BQ
    col = lax.broadcasted_iota(jnp.int32, shape, 1) + j * BK
    return (col <= row) & (col >= start)


def _lanes(op, value):
    out = value[:, 0:128]
    for t in range(1, value.shape[1] // 128):
        out = op(out, value[:, t * 128:(t + 1) * 128])
    return out


def _kdot(a, b):
    return lax.dot_general(a, b, (((1,), (1,)), ((), ())), preferred_element_type=jnp.float32)


def attn_fwd_kernel(head_dim, lo_ref, qkv_ref, start_ref, o_ref, lse_ref, k_scr, v_scr, strip, stat):
    i = pl.program_id(0)
    scale2 = head_dim ** -0.5 * math.log2(math.e)

    @pl.when(i == 0)
    def _():
        k_scr[...] = qkv_ref[:, head_dim:2 * head_dim]
        v_scr[...] = qkv_ref[:, 2 * head_dim:3 * head_dim]

    q = qkv_ref[pl.ds(pl.multiple_of(i * BQ, BQ), BQ), 0:head_dim]
    start = start_ref[...]
    lo = lo_ref[i]
    hi = (i * BQ + BQ - 1) // BK + 1

    def cols(j):
        return pl.ds(pl.multiple_of(j * BK, BK), BK)

    stat[...] = jnp.full_like(stat, NEG)

    @pl.loop(lo, hi)
    def _(j):
        s = jnp.where(_mask(i, j, start), _kdot(q, k_scr[cols(j), :]), NEG)
        strip[:, cols(j)] = s
        stat[...] = jnp.maximum(stat[...], _lanes(jnp.maximum, s))

    top = jnp.max(stat[...], axis=1, keepdims=True) * scale2
    stat[...] = jnp.zeros_like(stat)

    @pl.loop(lo, hi)
    def _(j):
        e = jnp.exp2(strip[:, cols(j)] * scale2 - top)
        strip[:, cols(j)] = e
        stat[...] += _lanes(jnp.add, e)

    total = jnp.sum(stat[...], axis=1, keepdims=True)
    inv = 1.0 / total

    def body(j, acc):
        p = (strip[:, cols(j)] * inv).astype(jnp.bfloat16)
        return acc + jnp.dot(p, v_scr[cols(j), :], preferred_element_type=jnp.float32)

    acc = lax.fori_loop(lo, hi, body, jnp.zeros((BQ, head_dim), jnp.float32))
    o_ref[...] = acc.astype(jnp.bfloat16)
    lse_ref[...] = top + jnp.log2(total)


def attn_fwd(qkv, start, lo):
    tokens = qkv.shape[0]
    head_dim = qkv.shape[1] // 3
    return pl.pallas_call(
        functools.partial(attn_fwd_kernel, head_dim),
        grid_spec=pltpu.PrefetchScalarGridSpec(
            num_scalar_prefetch=1,
            grid=(tokens // BQ,),
            in_specs=[pl.BlockSpec(qkv.shape, lambda i, lo: (0, 0)),
                      pl.BlockSpec((BQ, 1), lambda i, lo: (i, 0))],
            out_specs=[pl.BlockSpec((BQ, head_dim), lambda i, lo: (i, 0)),
                       pl.BlockSpec((BQ, 1), lambda i, lo: (i, 0))],
            scratch_shapes=[pltpu.VMEM((tokens, head_dim), jnp.bfloat16),
                            pltpu.VMEM((tokens, head_dim), jnp.bfloat16),
                            pltpu.VMEM((BQ, tokens), jnp.float32),
                            pltpu.VMEM((BQ, 128), jnp.float32)]),
        out_shape=[jax.ShapeDtypeStruct((tokens, head_dim), jnp.bfloat16),
                   jax.ShapeDtypeStruct((tokens, 1), jnp.float32)],
        compiler_params=pltpu.CompilerParams(vmem_limit_bytes=VMEM_LIMIT),
        cost_estimate=pl.CostEstimate(flops=4 * tokens * tokens * head_dim, bytes_accessed=4 * tokens * 1024,
                                      transcendentals=0),
        name="attn_fwd",
    )(lo, qkv, start)


def attn_bwd_kernel(head_dim, lo_ref, qkv_ref, do_ref, start_ref, lse_ref, out_ref,
                    k_scr, v_scr, p_strip, g_strip, stat, dk_scr, dv_scr):
    i = pl.program_id(0)
    scale = head_dim ** -0.5
    scale2 = scale * math.log2(math.e)

    @pl.when(i == 0)
    def _():
        k_scr[...] = qkv_ref[:, head_dim:2 * head_dim]
        v_scr[...] = qkv_ref[:, 2 * head_dim:3 * head_dim]
        dk_scr[...] = jnp.zeros_like(dk_scr)
        dv_scr[...] = jnp.zeros_like(dv_scr)

    rows = pl.ds(pl.multiple_of(i * BQ, BQ), BQ)
    q = qkv_ref[rows, 0:head_dim]
    do = do_ref[...]
    start = start_ref[...]
    lse = lse_ref[...]
    lo = lo_ref[i]
    hi = (i * BQ + BQ - 1) // BK + 1

    def cols(j):
        return pl.ds(pl.multiple_of(j * BK, BK), BK)

    stat[...] = jnp.zeros_like(stat)

    @pl.loop(lo, hi)
    def _(j):
        s = _kdot(q, k_scr[cols(j), :])
        p = jnp.where(_mask(i, j, start), jnp.exp2(s * scale2 - lse), 0.0)
        g = _kdot(do, v_scr[cols(j), :]).astype(jnp.bfloat16)
        p_strip[:, cols(j)] = p
        g_strip[:, cols(j)] = g
        stat[...] += _lanes(jnp.add, p * g.astype(jnp.float32))

    mean = jnp.sum(stat[...], axis=1, keepdims=True)
    q_t = q.astype(jnp.float32).T.astype(jnp.bfloat16)
    do_t = do.astype(jnp.float32).T.astype(jnp.bfloat16)

    def body(j, acc):
        p = p_strip[:, cols(j)]
        ds = (p * (g_strip[:, cols(j)].astype(jnp.float32) - mean)).astype(jnp.bfloat16)
        dk_scr[:, cols(j)] += jnp.dot(q_t, ds, preferred_element_type=jnp.float32)
        dv_scr[:, cols(j)] += jnp.dot(do_t, p.astype(jnp.bfloat16), preferred_element_type=jnp.float32)
        return acc + jnp.dot(ds, k_scr[cols(j), :], preferred_element_type=jnp.float32)

    dq = lax.fori_loop(lo, hi, body, jnp.zeros((BQ, head_dim), jnp.float32))
    out_ref[rows, 0:head_dim] = (dq * scale).astype(jnp.bfloat16)

    @pl.when(i == pl.num_programs(0) - 1)
    def _():
        @pl.loop(0, dk_scr.shape[1] // BK)
        def _(j):
            out_ref[cols(j), head_dim:2 * head_dim] = (dk_scr[:, cols(j)] * scale).T.astype(jnp.bfloat16)
            out_ref[cols(j), 2 * head_dim:3 * head_dim] = dv_scr[:, cols(j)].T.astype(jnp.bfloat16)


def attn_bwd(qkv, d_out, start, lse, lo):
    tokens = qkv.shape[0]
    head_dim = qkv.shape[1] // 3
    return pl.pallas_call(
        functools.partial(attn_bwd_kernel, head_dim),
        grid_spec=pltpu.PrefetchScalarGridSpec(
            num_scalar_prefetch=1,
            grid=(tokens // BQ,),
            in_specs=[pl.BlockSpec(qkv.shape, lambda i, lo: (0, 0)),
                      pl.BlockSpec((BQ, head_dim), lambda i, lo: (i, 0)),
                      pl.BlockSpec((BQ, 1), lambda i, lo: (i, 0)),
                      pl.BlockSpec((BQ, 1), lambda i, lo: (i, 0))],
            out_specs=pl.BlockSpec(qkv.shape, lambda i, lo: (0, 0)),
            scratch_shapes=[pltpu.VMEM((tokens, head_dim), jnp.bfloat16),
                            pltpu.VMEM((tokens, head_dim), jnp.bfloat16),
                            pltpu.VMEM((BQ, tokens), jnp.float32),
                            pltpu.VMEM((BQ, tokens), jnp.bfloat16),
                            pltpu.VMEM((BQ, 128), jnp.float32),
                            pltpu.VMEM((head_dim, tokens), jnp.float32),
                            pltpu.VMEM((head_dim, tokens), jnp.float32)]),
        out_shape=jax.ShapeDtypeStruct(qkv.shape, jnp.bfloat16),
        compiler_params=pltpu.CompilerParams(vmem_limit_bytes=VMEM_LIMIT),
        cost_estimate=pl.CostEstimate(flops=10 * tokens * tokens * head_dim, bytes_accessed=4 * tokens * 1024,
                                      transcendentals=0),
        name="attn_bwd",
    )(lo, qkv, d_out, start, lse)


def segment_starts(seg):
    bounds = [jnp.sum((seg < value).astype(jnp.int32)) for value in (1, 2, 3)]
    start = jnp.where(seg >= 3, bounds[2], jnp.where(seg >= 2, bounds[1], jnp.where(seg >= 1, bounds[0], 0)))
    return start[:, None], start[::BQ] // BK


def solution(mesh):
    groups = mesh.shape["model"]

    def normalize(values):
        values_f32 = values.astype(jnp.float32)
        centered = values_f32 - jnp.mean(values_f32, axis=-1, keepdims=True)
        inv_std = lax.rsqrt(jnp.mean(centered * centered, axis=-1, keepdims=True) + LN_EPS)
        return centered * inv_std, inv_std

    def norm_backward(grad_out, x_hat, inv_std, gain_vec):
        d_gain = jnp.sum(grad_out * x_hat, axis=0)
        d_hat = grad_out * gain_vec.astype(jnp.float32)
        d_in = inv_std * (d_hat - jnp.mean(d_hat, axis=-1, keepdims=True)
                          - x_hat * jnp.mean(d_hat * x_hat, axis=-1, keepdims=True))
        return d_in, d_gain

    def mm(spec, left, right):
        return jnp.einsum(spec, left, right, preferred_element_type=jnp.float32)

    def gather(rows):
        return lax.all_gather(rows, "model", axis=0, tiled=True)

    def scatter(rows):
        return lax.psum_scatter(rows, "model", scatter_dimension=0, tiled=True)

    def local_layer(act_x, seg_ids, gain_one, gain_two, w_qkv, w_out, w_up, w_down, grad_y):
        bf16 = jnp.bfloat16
        tokens, width = act_x.shape
        own = tokens // groups
        here = lax.axis_index("model") * own
        start, lo = segment_starts(seg_ids)
        w_out_all = gather(w_out.reshape(-1, width))

        normed_one, qkv = ln_qkv(act_x, gain_one, w_qkv)
        attn, lse = attn_fwd(qkv, start, lo)
        attn_own = lax.all_to_all(attn, "model", split_axis=0, concat_axis=1, tiled=True)
        x_own = lax.dynamic_slice_in_dim(act_x, here, own)
        dy_own = lax.dynamic_slice_in_dim(grad_y, here, own)
        resid_own = (x_own.astype(jnp.float32) + mm("sc,ce->se", attn_own, w_out_all)).astype(bf16)
        hat_two, inv_two = normalize(resid_own)
        normed_two = gather((hat_two * gain_two.astype(jnp.float32)).astype(bf16))

        act_vals, gelu_pull = jax.vjp(functools.partial(jax.nn.gelu, approximate=True),
                                      mm("sh,hf->sf", normed_two, w_up))
        hidden = act_vals.astype(bf16)
        d_hidden = mm("se,fe->sf", grad_y, w_down).astype(bf16)
        d_pre = gelu_pull(d_hidden.astype(jnp.float32))[0].astype(bf16)
        d_normed_two = scatter(mm("sf,hf->sh", d_pre, w_up).astype(bf16)).astype(jnp.float32)
        d_in_two, d_gain_two = norm_backward(d_normed_two, hat_two, inv_two, gain_two)
        d_resid = (dy_own.astype(jnp.float32) + d_in_two).astype(bf16)
        d_attn_own = mm("se,ce->sc", d_resid, w_out_all).astype(bf16)
        d_attn = lax.all_to_all(d_attn_own, "model", split_axis=1, concat_axis=0, tiled=True)

        sum_two = scatter(mm("sf,fe->se", hidden, w_down).astype(bf16))
        layer_out = gather((resid_own.astype(jnp.float32) + sum_two.astype(jnp.float32)).astype(bf16))

        d_qkv = attn_bwd(qkv, d_attn, start, lse, lo)
        d_normed_one = scatter(mm("sc,hc->sh", d_qkv, w_qkv).astype(bf16)).astype(jnp.float32)
        hat_one, inv_one = normalize(x_own)
        d_in_one, d_gain_one = norm_backward(d_normed_one, hat_one, inv_one, gain_one)
        grad_x = gather((d_resid.astype(jnp.float32) + d_in_one).astype(bf16))
        d_gains = lax.psum(jnp.stack([d_gain_one, d_gain_two]), "model").astype(bf16)

        d_wout = mm("sd,se->de", attn, gather(d_resid)).astype(bf16).reshape(w_out.shape)
        d_down = mm("sf,se->fe", hidden, grad_y).astype(bf16)
        d_up = mm("sh,sf->hf", normed_two, d_pre).astype(bf16)
        d_wqkv = mm("sh,sc->hc", normed_one, d_qkv).astype(bf16)
        return layer_out, grad_x, d_wqkv, d_wout, d_up, d_down, d_gains[0], d_gains[1]

    in_specs = (P("data", None), P("data"), P(None), P(None), P(None, "model"),
                P("model", None, None), P(None, "model"), P("model", None), P("data", None))
    out_specs = (P("data", None), P("data", None), P("data", "model"), P(("data", "model"), None, None),
                 P("data", "model"), P(("data", "model"), None), P("data"), P("data"))
    return jax.shard_map(local_layer, mesh=mesh, in_specs=in_specs, out_specs=out_specs, check_vma=False)
```
